32 devices in a mesh: ep: 16 (over z, x, core), dp: 2 (over y).
Axes of the slice: x: 2, y: 2, z: 4, core: 2. Of those that a mesh axis runs over, the one named last changes fastest.
Arguments:
- tokens: bfloat16 [4096, 2048], P(('dp', 'ep')), parts along dimension 0, may hold values from -6 to 6
- expert_ids: int32 [4096, 8], P(('dp', 'ep')), parts along dimension 0, may hold values from 0 to 15, all different within a row; in each aligned block of 128 rows (0 to 127, 128 to 255, ...) at most 96 rows name the same one
- route_logits: float32 [4096, 8], P(('dp', 'ep')), parts along dimension 0, may hold values from -3 to 300
- w_gate: bfloat16 [16, 2048, 1024], P('ep'), may hold values from -0.125 to 0.125
- w_up: bfloat16 [16, 2048, 1024], P('ep'), may hold values from -0.125 to 0.125
- w_down: bfloat16 [16, 1024, 2048], P('ep'), may hold values from -0.1875 to 0.1875
Outputs:
- mixed_rows: bfloat16 [4096, 2048], P(('dp', 'ep')), parts along dimension 0
The draws below stay inside these ranges and needn't reach their ends.
There are 2 independent parts, one for each index of `dp`. The reference program is written for one: setup_inputs(seed, part) draws one part's arguments, and reference() takes and returns one part's arrays. A program takes and returns all parts, laid end to end along the dimension named above; an argument that names none is the same for every part. Nothing has to cross between parts.
Inputs may be any that keep to these rules, and one draw needn't show every extreme that they name: `expert_ids`: each row names 8 different experts; among the 128 rows of one device no expert is named more than 96 times, a bound that some block reaches.
All inputs are finite; a program needn't handle non-finite values.
Results may differ from the reference program's by a relative error of at most 0.0058.
Values may be sent and summed in bfloat16 or wider, within the bound.
No kernel may reach another device: no remote copies, remote signals or barrier semaphores. Data moves between devices by JAX's collectives and lax.ppermute only.
A program may use at most 128 MiB of HBM per device.

```python
import math
import jax
import jax.numpy as jnp
import numpy as np
from jax import lax

D = 2048
FF = 1024
TOP = 8
TOK_DEV = 128
EXPERTS = 16
TOKENS = 2048
CAP = 96
N_EP = 16


def draw_route_logits(key, part):
    first_key = jax.random.fold_in(key, 11)
    values = jnp.clip(jax.random.normal(first_key, (TOKENS, TOP), jnp.float32) * 0.4, -0.75, 0.75)
    return values


def block_scale(key, extent, shards, smallest, top_value):
    loudness, own = 1.0, jax.random.fold_in(key, 6)
    for dim, shards_of in shards:
        steps = jnp.exp(jax.random.uniform(jax.random.fold_in(own, dim), (shards_of,), jnp.float32, smallest / len(shards), top_value / len(shards)))
        loudness = loudness * jnp.repeat(steps, extent[dim] // shards_of).reshape([-1 if axis == dim else 1 for axis in range(len(extent))])
    return loudness


def shared_out(stream_key, own, number, rows, number_of, top, bound, skew):
    ranking = jax.random.permutation(stream_key, number_of)
    packed, ordinary = shares(number_of, rows * top, bound, skew, True), shares(number_of, rows * top, bound, skew, False)
    places = jnp.arange(number_of)

    def named(sizes, turn):
        used = int((sizes > 0).sum())
        fixed = max(1, used // 4)
        moved = fixed + (places - fixed + turn * (used - fixed)) % max(1, number_of - fixed)
        return jnp.zeros((number_of,), jnp.int32).at[ranking[jnp.where(places < fixed, places, moved)]].set(jnp.asarray(sizes, jnp.int32))

    sizes = jnp.where(number % 4 == 0, named(packed, number // 4), named(ordinary, number - number // 4 - 1))
    mixed = jax.random.permutation(jax.random.fold_in(own, 3), number_of)
    source_of, sink = mixed[0:number_of // 2 * 2:2], mixed[1:number_of // 2 * 2:2]
    slack = jnp.minimum(sizes[source_of] - 1, bound - sizes[sink]) // 2
    slack = jnp.where((source_of == ranking[0]) | (sink == ranking[0]) | (sizes[sink] == 0), 0, jnp.maximum(slack, 0))
    moved = jax.random.randint(jax.random.fold_in(own, 4), (number_of // 2,), 0, 1 << 20) % (slack + 1)
    sizes = sizes.at[source_of].add(-moved).at[sink].add(moved)
    members = jnp.searchsorted(jnp.cumsum(sizes), jnp.arange(rows * top), side="right").astype(jnp.int32)
    grid = members.reshape(top, rows).T
    grid = grid[jax.random.permutation(jax.random.fold_in(own, 1), rows)]
    turn = jax.random.randint(jax.random.fold_in(own, 2), (rows, 1), 0, top)
    return jnp.take_along_axis(grid, (jnp.arange(top)[None, :] + turn) % top, axis=1)


def shares(count, total, bound, skew, full):
    loads = [(1 << 20) // math.isqrt(grade ** skew) + 1 for grade in range(1, count + 1)]
    largest = bound if full else min(bound, max(-(-total // count), total * loads[0] // sum(loads)))
    least = 1 if total - largest >= count - 1 else 0
    given, rest = [largest] + [least] * (count - 1), total - largest - least * (count - 1)
    while rest > 0:
        movable = [i for i in range(1, count) if given[i] < largest] or [i for i in range(1, count) if given[i] < bound]
        pool, left = sum([loads[i] for i in movable]), rest
        for i in movable:
            more = min(bound - given[i], max(1, left * loads[i] // pool), rest)
            given[i] = given[i] + more
            rest = rest - more
    return np.array(given)


def centred(own_key, extent, scale, bound, pieces=(), kind=jnp.bfloat16):
    values = jax.random.normal(own_key, extent, jnp.float32) * scale
    if len(pieces) > 0:
        values = block_scale(own_key, extent, pieces, -0.22, 0.18) * values
    return jnp.clip(values, min=-bound, max=bound).astype(kind)


def setup_inputs(seed: int = 0, part: int = 0) -> dict:
    key_list = jax.random.split(jax.random.key(seed), 7)
    part_keys = jax.random.split(jax.random.fold_in(key_list[6], part), 7)
    tokens = centred(part_keys[0], (TOKENS, D), 1.0, 6.0, ((0, 16),))
    expert_ids_keys = jax.random.split(jax.random.fold_in(part_keys[1], 1), TOKENS // TOK_DEV)
    expert_ids_turns = jax.random.permutation(jax.random.fold_in(part_keys[1], 3), TOKENS // TOK_DEV)
    expert_ids = jax.vmap(lambda own, number: shared_out(jax.random.fold_in(part_keys[1], 2), own, number, TOK_DEV, EXPERTS, TOP, CAP, 2))(expert_ids_keys, expert_ids_turns).reshape((TOKENS, TOP))
    route_logits = draw_route_logits(jax.random.fold_in(jax.random.fold_in(key_list[6], part), 71), part)
    w_gate = centred(key_list[3], (EXPERTS, D, FF), D ** -0.5, 0.125, ((0, 16),))
    w_up = centred(key_list[4], (EXPERTS, D, FF), D ** -0.5, 0.125, ((0, 16),))
    w_down = centred(key_list[5], (EXPERTS, FF, D), FF ** -0.5, 0.1875, ((0, 16),))
    return {"tokens": tokens, "expert_ids": expert_ids, "route_logits": route_logits, "w_gate": w_gate, "w_up": w_up, "w_down": w_down}


def expert_ffn(rows, gate_weight, up_weight, down_weight):
    gate = jnp.dot(rows, gate_weight, preferred_element_type=jnp.float32)
    up_part = jnp.dot(rows, up_weight, preferred_element_type=jnp.float32)
    hidden = (jax.nn.silu(gate) * up_part).astype(jnp.bfloat16)
    return jnp.dot(hidden, down_weight, preferred_element_type=jnp.float32).astype(jnp.bfloat16)


def reference(tokens, expert_ids, route_logits, w_gate, w_up, w_down):
    token_count, model_width = tokens.shape
    picks = expert_ids.shape[1]
    gates = jax.nn.softmax(route_logits.astype(jnp.float32), axis=-1)
    flat_ids = expert_ids.reshape(-1)
    flat_gates = gates.reshape(-1)
    flat_token = (jnp.arange(token_count * picks, dtype=jnp.int32) // picks).astype(jnp.int32)
    buffer = N_EP * CAP
    padded = jnp.concatenate([tokens, jnp.zeros((1, model_width), tokens.dtype)], 0)

    def expert_pass(mixed, inputs):
        gate_weight, up_weight, down_weight, expert = inputs
        chosen = flat_ids == expert
        place = (jnp.cumsum(chosen.astype(jnp.int32)) - 1).astype(jnp.int32)
        target = jnp.where(chosen, place, buffer).astype(jnp.int32)
        rows_token = jnp.full((buffer,), token_count, jnp.int32).at[target].set(flat_token, mode="drop")
        rows_gate = jnp.zeros((buffer,), jnp.float32).at[target].set(flat_gates, mode="drop")
        answer = expert_ffn(padded[rows_token], gate_weight, up_weight, down_weight)
        mixed = mixed.at[rows_token].add(rows_gate[:, None] * answer.astype(jnp.float32), mode="drop")
        return mixed, None

    start = jnp.zeros((token_count, model_width), jnp.float32)
    mixed, _ = lax.scan(expert_pass, start, (w_gate, w_up, w_down, jnp.arange(EXPERTS, dtype=jnp.int32)))
    return mixed.astype(jnp.bfloat16)
```

```python
import functools

import jax
import jax.numpy as jnp
import numpy as np
from jax import lax
from jax.experimental import pallas as pl
from jax.experimental.pallas import tpu as pltpu
from jax.sharding import PartitionSpec as P


def chip_cycle(mesh):
    axis = mesh.axis_names.index("ep")
    line = np.moveaxis(mesh.devices, axis, 0).reshape(mesh.shape["ep"], -1)[:, 0]
    groups = {}
    for place, device in enumerate(line):
        coords = tuple(getattr(device, "coords", None) or (place // 2,))
        groups.setdefault(coords, []).append(place)
    spots = list(groups)
    varying = [d for d in range(len(spots[0])) if len({s[d] for s in spots}) > 1]
    ordered = sorted(spots)
    if len(varying) == 2:
        first, second = varying
        if len({s[first] for s in spots}) % 2:
            first, second = second, first
        if len({s[first] for s in spots}) < len({s[second] for s in spots}) and len({s[second] for s in spots}) % 2 == 0:
            first, second = second, first
        rows = sorted({s[first] for s in spots})
        cols = sorted({s[second] for s in spots})
        path = []
        for number, row in enumerate(rows):
            inner = cols[1:] if number % 2 == 0 else cols[1:][::-1]
            path += [(row, col) for col in inner]
        path += [(row, cols[0]) for row in reversed(rows)]
        by_pair = {(s[first], s[second]): s for s in spots}
        ordered = [by_pair[pair] for pair in path]
    return [groups[s] for s in ordered]


def ffn_body(pieces, *refs):
    x_refs = refs[:pieces]
    scale_ref, gate_ref, up_ref, down_ref = refs[pieces : pieces + 4]
    out_refs = refs[pieces + 4 : 2 * pieces + 4]
    x_all, total = refs[2 * pieces + 4 :]
    turn = pl.program_id(0)

    @pl.when(turn == 0)
    def _():
        first = 0
        for x_ref in x_refs:
            x_all[first : first + x_ref.shape[0], :] = x_ref[...]
            first += x_ref.shape[0]

    x = x_all[...]
    gate = jnp.dot(x, gate_ref[0], preferred_element_type=jnp.float32)
    up_part = jnp.dot(x, up_ref[0], preferred_element_type=jnp.float32)
    hidden = (gate / (1.0 + jnp.exp(-gate)) * up_part).astype(jnp.bfloat16)
    part = jnp.dot(hidden, down_ref[0], preferred_element_type=jnp.float32)

    @pl.when(turn == 0)
    def _():
        total[...] = part

    @pl.when(turn > 0)
    def _():
        total[...] += part

    @pl.when(turn == pl.num_programs(0) - 1)
    def _():
        first = 0
        for out_ref in out_refs:
            span = slice(first, first + out_ref.shape[0])
            out_ref[...] = (total[span, :] * scale_ref[span, :]).astype(jnp.bfloat16)
            first += out_ref.shape[0]


def expert_rows(xs, scale, w_gate, w_up, w_down):
    rows = sum(x.shape[0] for x in xs)
    width = xs[0].shape[1]
    hidden_width = w_gate.shape[2]
    block = min(256, hidden_width)
    whole = lambda shape: pl.BlockSpec(shape, lambda j: (0, 0))
    return pl.pallas_call(
        functools.partial(ffn_body, len(xs)),
        grid=(hidden_width // block,),
        in_specs=[whole(x.shape) for x in xs]
        + [
            whole(scale.shape),
            pl.BlockSpec((1, width, block), lambda j: (0, 0, j)),
            pl.BlockSpec((1, width, block), lambda j: (0, 0, j)),
            pl.BlockSpec((1, block, width), lambda j: (0, j, 0)),
        ],
        out_specs=[whole(x.shape) for x in xs],
        out_shape=[jax.ShapeDtypeStruct(x.shape, jnp.bfloat16) for x in xs],
        scratch_shapes=[
            pltpu.VMEM((rows, width), jnp.bfloat16),
            pltpu.VMEM((rows, width), jnp.float32),
        ],
        cost_estimate=pl.CostEstimate(
            flops=6 * rows * width * hidden_width,
            bytes_accessed=6 * width * hidden_width + 4 * rows * width,
            transcendentals=rows * hidden_width,
        ),
        compiler_params=pltpu.CompilerParams(dimension_semantics=("arbitrary",)),
    )(*xs, scale, w_gate, w_up, w_down)


def per_device(cycle, tokens, expert_ids, route_logits, w_gate, w_up, w_down):
    chips = len(cycle)
    half_way = chips // 2
    experts = lax.axis_size("ep")
    tok_rows, _ = tokens.shape
    half = tok_rows // 2
    forth = [(cycle[c][k], cycle[(c + 1) % chips][k]) for c in range(chips) for k in range(2)]
    back = [(b, a) for a, b in forth]
    swap = [(pair[k], pair[1 - k]) for pair in cycle for k in range(2)]
    cw = lambda v: lax.ppermute(v, "ep", forth)
    ccw = lambda v: lax.ppermute(v, "ep", back)
    mate = lambda v: lax.ppermute(v, "ep", swap)

    gates = jax.nn.softmax(route_logits.astype(jnp.float32), axis=-1)
    names = jnp.arange(experts, dtype=jnp.int32)
    spread = jnp.sum(
        jnp.where(expert_ids.T[None, :, :] == names[:, None, None], gates.T[None, :, :], 0.0), axis=1
    )
    all_gates = lax.all_to_all(spread, "ep", split_axis=0, concat_axis=0, tiled=True)

    table = np.zeros((experts, 2 * chips), np.int32)
    for c in range(chips):
        for k in range(2):
            seen = [cycle[c][k], cycle[c][1 - k]]
            for s in range(1, half_way):
                before, after = cycle[(c - s) % chips], cycle[(c + s) % chips]
                seen += [before[k], after[k], before[1 - k], after[1 - k]]
            opposite = cycle[(c + half_way) % chips]
            table[cycle[c][k]] = seen + [opposite[k], opposite[1 - k]]
    order = lax.dynamic_index_in_dim(jnp.asarray(table), lax.axis_index("ep"), 0, keepdims=False)
    scales = all_gates[order].reshape(experts * tok_rows, 1)

    def answers(xs, first):
        rows = sum(x.shape[0] for x in xs)
        return expert_rows(xs, lax.slice_in_dim(scales, first, first + rows), w_gate, w_up, w_down)

    ahead, behind = tokens, tokens
    arrived = [[tokens, mate(tokens)]]
    for s in range(1, half_way):
        ahead, behind = cw(ahead), ccw(behind)
        arrived.append([ahead, behind, mate(ahead), mate(behind)])
    ahead, behind = cw(ahead[:half]), ccw(behind[half:])
    arrived.append([ahead, behind, mate(ahead), mate(behind)])

    results, first = [], 0
    for xs in arrived:
        results.append(answers(xs, first))
        first += sum(x.shape[0] for x in xs)

    wide = lambda v: v.astype(jnp.float32)
    own_f, own_b, far_f, far_b = results[half_way]
    to_back = (wide(own_f) + wide(mate(far_f))).astype(jnp.bfloat16)
    to_front = (wide(own_b) + wide(mate(far_b))).astype(jnp.bfloat16)
    for s in range(half_way - 1, 0, -1):
        own_f, own_b, far_f, far_b = results[s]
        sum_f = wide(own_f) + wide(mate(far_f))
        sum_b = wide(own_b) + wide(mate(far_b))
        got_f, got_b = wide(ccw(to_back)), wide(cw(to_front))
        if s == half_way - 1:
            got_f = jnp.pad(got_f, ((0, tok_rows - half), (0, 0)))
            got_b = jnp.pad(got_b, ((half, 0), (0, 0)))
        to_back = (sum_f + got_f).astype(jnp.bfloat16)
        to_front = (sum_b + got_b).astype(jnp.bfloat16)
    got_f, got_b = wide(ccw(to_back)), wide(cw(to_front))
    if half_way == 1:
        got_f = jnp.pad(got_f, ((0, tok_rows - half), (0, 0)))
        got_b = jnp.pad(got_b, ((half, 0), (0, 0)))
    own, far = results[0]
    return (wide(own) + wide(mate(far)) + got_f + got_b).astype(jnp.bfloat16)


def solution(mesh):
    in_specs = (
        P(("dp", "ep"), None),
        P(("dp", "ep"), None),
        P(("dp", "ep"), None),
        P("ep", None, None),
        P("ep", None, None),
        P("ep", None, None),
    )
    out_specs = P(("dp", "ep"), None)
    return jax.shard_map(
        functools.partial(per_device, chip_cycle(mesh)),
        mesh=mesh, in_specs=in_specs, out_specs=out_specs, check_vma=False,
    )
```

```python
import functools

import jax
import jax.numpy as jnp
import numpy as np
from jax import lax
from jax.experimental import pallas as pl
from jax.experimental.pallas import tpu as pltpu
from jax.sharding import PartitionSpec as P


def chip_cycle(mesh):
    axis = mesh.axis_names.index("ep")
    line = np.moveaxis(mesh.devices, axis, 0).reshape(mesh.shape["ep"], -1)[:, 0]
    groups = {}
    for place, device in enumerate(line):
        coords = tuple(getattr(device, "coords", None) or (place // 2,))
        groups.setdefault(coords, []).append(place)
    spots = list(groups)
    varying = [d for d in range(len(spots[0])) if len({s[d] for s in spots}) > 1]
    ordered = sorted(spots)
    if len(varying) == 2:
        first, second = varying
        if len({s[first] for s in spots}) % 2:
            first, second = second, first
        if len({s[first] for s in spots}) < len({s[second] for s in spots}) and len({s[second] for s in spots}) % 2 == 0:
            first, second = second, first
        rows = sorted({s[first] for s in spots})
        cols = sorted({s[second] for s in spots})
        path = []
        for number, row in enumerate(rows):
            inner = cols[1:] if number % 2 == 0 else cols[1:][::-1]
            path += [(row, col) for col in inner]
        path += [(row, cols[0]) for row in reversed(rows)]
        by_pair = {(s[first], s[second]): s for s in spots}
        ordered = [by_pair[pair] for pair in path]
    return [groups[s] for s in ordered]


def ffn_body(pieces, ups, *refs):
    x_refs = refs[:pieces]
    scale_ref, gate_ref, up_ref, down_ref = refs[pieces : pieces + 4]
    out_refs = refs[pieces + 4 : 2 * pieces + 4]
    x_all, hidden, column = refs[2 * pieces + 4 :]
    turn = pl.program_id(0)

    @pl.when(turn == 0)
    def _():
        first = 0
        for x_ref in x_refs:
            x_all[first : first + x_ref.shape[0], :] = x_ref[...]
            first += x_ref.shape[0]
        for row in range(scale_ref.shape[0]):
            line = jnp.broadcast_to(scale_ref[row : row + 1, :], (128, 128))
            column[row * 128 : (row + 1) * 128, :] = line.T

    @pl.when(turn < ups)
    def _():
        x = x_all[...]
        gate = jnp.dot(x, gate_ref[0], preferred_element_type=jnp.float32)
        up_part = jnp.dot(x, up_ref[0], preferred_element_type=jnp.float32)
        hidden[turn] = (gate / (1.0 + jnp.exp(-gate)) * up_part).astype(jnp.bfloat16)

    @pl.when(turn >= ups)
    def _():
        full = jnp.concatenate([hidden[i] for i in range(ups)], axis=1)
        part = jnp.dot(full, down_ref[0], preferred_element_type=jnp.float32)
        part = (part * column[:, :1]).astype(jnp.bfloat16)
        first = 0
        for out_ref in out_refs:
            out_ref[...] = part[first : first + out_ref.shape[0], :]
            first += out_ref.shape[0]


def expert_rows(xs, scale, w_gate, w_up, w_down, block=256, wide_block=1024):
    rows = sum(x.shape[0] for x in xs)
    width = xs[0].shape[1]
    hidden_width = w_gate.shape[2]
    block, wide_block = min(block, hidden_width), min(wide_block, width)
    ups = hidden_width // block
    whole = lambda shape: pl.BlockSpec(shape, lambda j: (0, 0))
    to_hidden = pl.BlockSpec((1, width, block), lambda j: (0, 0, jnp.minimum(j, ups - 1)))
    return pl.pallas_call(
        functools.partial(ffn_body, len(xs), ups),
        grid=(ups + width // wide_block,),
        in_specs=[whole(x.shape) for x in xs]
        + [
            whole(scale.shape),
            to_hidden,
            to_hidden,
            pl.BlockSpec((1, hidden_width, wide_block), lambda j: (0, 0, jnp.maximum(j - ups, 0))),
        ],
        out_specs=[
            pl.BlockSpec((x.shape[0], wide_block), lambda j: (0, jnp.maximum(j - ups, 0))) for x in xs
        ],
        out_shape=[jax.ShapeDtypeStruct(x.shape, jnp.bfloat16) for x in xs],
        scratch_shapes=[
            pltpu.VMEM((rows, width), jnp.bfloat16),
            pltpu.VMEM((ups, rows, block), jnp.bfloat16),
            pltpu.VMEM((rows, 128), jnp.float32),
        ],
        cost_estimate=pl.CostEstimate(
            flops=6 * rows * width * hidden_width,
            bytes_accessed=6 * width * hidden_width + 4 * rows * width,
            transcendentals=rows * hidden_width,
        ),
        compiler_params=pltpu.CompilerParams(dimension_semantics=("arbitrary",)),
    )(*xs, scale, w_gate, w_up, w_down)


def layer(cycle, tokens, expert_ids, route_logits, w_gate, w_up, w_down):
    chips = len(cycle)
    half_way = chips // 2
    experts = lax.axis_size("ep")
    tok_rows, _ = tokens.shape
    half = tok_rows // 2
    forth = [(cycle[c][k], cycle[(c + 1) % chips][k]) for c in range(chips) for k in range(2)]
    back = [(b, a) for a, b in forth]
    swap = [(pair[k], pair[1 - k]) for pair in cycle for k in range(2)]

    def cw(v):
        return lax.ppermute(v, "ep", forth)

    def ccw(v):
        return lax.ppermute(v, "ep", back)

    def mate(v):
        return lax.ppermute(v, "ep", swap)

    gates = jax.nn.softmax(route_logits.astype(jnp.float32), axis=-1)
    names = jnp.arange(experts, dtype=jnp.int32)
    spread = jnp.sum(
        jnp.where(expert_ids.T[None, :, :] == names[:, None, None], gates.T[None, :, :], 0.0), axis=1
    )
    all_gates = lax.all_to_all(spread, "ep", split_axis=0, concat_axis=0, tiled=True)

    table = np.zeros((experts, 2 * chips), np.int32)
    for c in range(chips):
        for k in range(2):
            seen = [cycle[c][k], cycle[c][1 - k]]
            for s in range(1, half_way):
                before, after = cycle[(c - s) % chips], cycle[(c + s) % chips]
                seen += [before[k], after[k], before[1 - k], after[1 - k]]
            opposite = cycle[(c + half_way) % chips]
            table[cycle[c][k]] = seen + [opposite[k], opposite[1 - k]]
    order = lax.dynamic_index_in_dim(jnp.asarray(table), lax.axis_index("ep"), 0, keepdims=False)
    scales = all_gates[order].reshape(experts * tok_rows // 128, 128)

    def answers(xs, first):
        rows = sum(x.shape[0] for x in xs)
        scale = lax.slice_in_dim(scales, first // 128, (first + rows) // 128)
        return expert_rows(xs, scale, w_gate, w_up, w_down)

    ahead, behind = tokens, tokens
    arrived = [[tokens, mate(tokens)]]
    for _ in range(1, half_way):
        ahead, behind = cw(ahead), ccw(behind)
        arrived.append([ahead, behind, mate(ahead), mate(behind)])
    ahead, behind = cw(ahead[:half]), ccw(behind[half:])
    far_ahead, far_behind = mate(ahead), mate(behind)
    arrived.append([ahead, behind, far_ahead, far_behind])

    results, first = [], 0
    for xs in arrived:
        results.append(answers(xs, first))
        first += sum(x.shape[0] for x in xs)

    wide = lambda v: v.astype(jnp.float32)
    own_f, own_b, far_f, far_b = results[half_way]
    to_back = (wide(own_f) + wide(mate(far_f))).astype(jnp.bfloat16)
    to_front = (wide(own_b) + wide(mate(far_b))).astype(jnp.bfloat16)
    for s in range(half_way - 1, 0, -1):
        own_f, own_b, far_f, far_b = results[s]
        sum_f = wide(own_f) + wide(mate(far_f))
        sum_b = wide(own_b) + wide(mate(far_b))
        got_f = wide(ccw(to_back))
        got_b = wide(cw(to_front))
        if s == half_way - 1:
            got_f = jnp.pad(got_f, ((0, tok_rows - half), (0, 0)))
            got_b = jnp.pad(got_b, ((half, 0), (0, 0)))
        to_back = (sum_f + got_f).astype(jnp.bfloat16)
        to_front = (sum_b + got_b).astype(jnp.bfloat16)
    got_f, got_b = wide(ccw(to_back)), wide(cw(to_front))
    if half_way == 1:
        got_f = jnp.pad(got_f, ((0, tok_rows - half), (0, 0)))
        got_b = jnp.pad(got_b, ((half, 0), (0, 0)))
    own, far = results[0]
    return (wide(own) + wide(mate(far)) + got_f + got_b).astype(jnp.bfloat16)


def per_device(cycle, *args):
    return layer(cycle, *args)


def solution(mesh):
    in_specs = (
        P(("dp", "ep"), None),
        P(("dp", "ep"), None),
        P(("dp", "ep"), None),
        P("ep", None, None),
        P("ep", None, None),
        P("ep", None, None),
    )
    out_specs = P(("dp", "ep"), None)
    cycle = chip_cycle(mesh)
    return jax.shard_map(
        functools.partial(per_device, cycle),
        mesh=mesh, in_specs=in_specs, out_specs=out_specs, check_vma=False,
    )
```
